32 devices in a mesh: gx: 4 (over z), gy: 8 (over y, x, core).
Axes of the slice: x: 2, y: 2, z: 4, core: 2. Of those that a mesh axis runs over, the one named last changes fastest.
Arguments:
- tokens: bfloat16 [2048, 6144], P('gy', 'gx'), may hold values from -7.5 to 7.5, as said below
- norm_gain: float32 [6144], P('gx'), may hold values from 0.1 to 1.9
- joined_weight: bfloat16 [6144, 43008], P('gx', 'gy'), may hold values from -0.078125 to 0.078125
Outputs:
- projected: bfloat16 [256, 8, 43008], P('gx', None, 'gy')
The draws below stay inside these ranges and needn't reach their ends.
Inputs may be any that keep to these rules, and one draw needn't show every extreme that they name: Every entry of tokens lies between -7.5 and 7.5; each token's features are noise plus an offset of its own plus a slope of its own times a ramp from -1 to 1 over the 6144 features.
All inputs are finite; a program needn't handle non-finite values.
Results may differ from the reference program's by a relative error of at most 0.014.
Values may be sent and summed in bfloat16 or wider, within the bound.
A program may use at most 128 MiB of HBM per device.

```python
import jax
import jax.numpy as jnp
from jax import lax

D = 6144
F = 43008
TOK_DEV = 256
TOKENS = 2048
N_GX = 4
N_GY = 8


def draw_tokens(key, part):
    noise_key = jax.random.fold_in(key, 11)
    offset_key = jax.random.fold_in(key, 12)
    slope_key = jax.random.fold_in(key, 13)
    noise = jnp.clip(jax.random.normal(noise_key, (TOKENS, D), jnp.float32), -4.0, 4.0)
    offset = jnp.clip(0.5 * jax.random.normal(offset_key, (TOKENS, 1), jnp.float32), -2.0, 2.0)
    slope = jax.random.uniform(slope_key, (TOKENS, 1), jnp.float32, -1.5, 1.5)
    ramp = (2.0 * jnp.arange(D, dtype=jnp.float32) + 1.0) / D - 1.0
    values = noise + offset + slope * ramp[None, :]
    return jnp.clip(values, -7.5, 7.5).astype(jnp.bfloat16)


def block_levels(key, shape, pieces, low, largest):
    def one(axis_at, shards_of):
        draws = jax.random.uniform(jax.random.fold_in(jax.random.fold_in(key, 6), axis_at), (shards_of,), jnp.float32, low / len(pieces), largest / len(pieces))
        return jnp.repeat(jnp.exp(draws), shape[axis_at] // shards_of).reshape((-1,) + (1,) * (len(shape) - axis_at - 1))

    level = one(*pieces[0])
    for cut in pieces[1:]:
        level = level * one(*cut)
    return level


def bell_draw(key, extent, spread, bound, shards=(), held_as=jnp.bfloat16):
    values = spread * jax.random.normal(key, extent, jnp.float32)
    if shards:
        values = values * block_levels(key, extent, shards, -0.22, 0.18)
    return jnp.clip(values, -bound, bound).astype(held_as)


def setup_inputs(seed: int = 0) -> dict:
    key_of = jax.random.split(jax.random.key(seed), 4)
    return {
        "tokens": draw_tokens(jax.random.fold_in(key_of[3], 71), 0),
        "norm_gain": jnp.clip(1.0 + 0.18 * jax.random.normal(key_of[1], (D,), jnp.float32), 0.1, 1.9),
        "joined_weight": bell_draw(key_of[2], (D, F), D ** -0.5, 0.078125, ((0, 4), (1, 8))),
    }


epsilon = 1e-06

def reference(tokens, norm_gain, joined_weight):
    values = tokens.astype(jnp.float32)
    mean = lax.optimization_barrier(jnp.sum(values, axis=1, keepdims=True)) / D
    centered = values - mean
    variance = lax.optimization_barrier(jnp.sum(centered * centered, axis=1, keepdims=True)) / D
    normed = (centered * lax.rsqrt(variance + epsilon) * norm_gain).astype(jnp.bfloat16)
    block_width = D // N_GX
    total = jnp.zeros((normed.shape[0], joined_weight.shape[1]), jnp.float32)
    for block in range(N_GX):
        lower = block * block_width
        term = jnp.dot(normed[:, lower:lower + block_width], joined_weight[lower:lower + block_width, :], preferred_element_type=jnp.float32)
        rounded = lax.optimization_barrier(term.astype(jnp.bfloat16))
        total = total + rounded.astype(jnp.float32)
    whole = total.astype(jnp.bfloat16)
    return jnp.transpose(whole.reshape(N_GY, TOK_DEV, whole.shape[1]), (1, 0, 2))
```

```python
import functools

import jax
import jax.numpy as jnp
from jax import lax
from jax.experimental import pallas as pl
from jax.experimental.pallas import tpu as pltpu
from jax.sharding import PartitionSpec as P

MESH = pl.DeviceIdType.MESH
EPSILON = 1e-06
STAGES = 4


def partner(y, step, ny):
    out, bit = 0, 1
    while bit < ny:
        out = out + bit * ((y // bit + step // bit) % 2)
        bit *= 2
    return out


def kernel(n, ny, width, tok_ref, gain_hbm, w_hbm, out_ref, w_s, gat, gain_s, stat, recv, acc, stg,
           cen, coef, gw, fin, tok_sem, gain_sem, w_sem, stat_send, stat_recv, gw_send, gw_recv, gat_send, gat_recv,
           send_sem, recv_sem):
    z, y = lax.axis_index("gx"), lax.axis_index("gy")
    tok, depth = tok_ref.shape
    part = tok // n
    stages = stg.shape[0]
    slots = recv.shape[1]
    columns = w_hbm.shape[1]
    tiles = columns // width
    chunks = ny * tiles
    ring = acc.shape[0]
    model = depth * n

    def cols(tile):
        if tiles == 1:
            return slice(None)
        return pl.ds(pl.multiple_of(tile * width, 128), width)

    def w_copy(tile):
        return pltpu.make_async_copy(w_hbm.at[:, cols(tile)], w_s.at[tile], w_sem.at[tile])

    tok_copy = pltpu.make_async_copy(tok_ref, gat.at[0], tok_sem)
    tok_copy.start()
    gain_copy = pltpu.make_async_copy(gain_hbm, gain_s, gain_sem)
    gain_copy.start()
    w_copy(0).start()

    barrier = pltpu.get_barrier_semaphore()
    for k in range(1, n):
        pl.semaphore_signal(barrier, inc=1, device_id=((z + k) % n, y), device_id_type=MESH)
    for k in range(1, ny):
        pl.semaphore_signal(barrier, inc=1, device_id=(z, partner(y, k, ny)), device_id_type=MESH)

    def gain_row():
        return gain_s[...].reshape(1, depth)

    tok_copy.wait()
    values = gat[0].astype(jnp.float32)
    total = jnp.sum(values, axis=1, keepdims=True)
    off = values - total / depth
    squares = jnp.sum(off * off, axis=1, keepdims=True)
    lane = lax.broadcasted_iota(jnp.int32, (tok, 128), 1)
    packed = jnp.where(lane == 0, total, squares)
    stat[z] = packed.T[:8]

    gain_copy.wait()
    cen[...] = (off * gain_row()).astype(jnp.bfloat16)

    pl.semaphore_wait(barrier, n - 1 + ny - 1)

    def across(ref, send, get, k, slot):
        return pltpu.make_async_remote_copy(
            src_ref=ref.at[slot], dst_ref=ref.at[slot], send_sem=send.at[k], recv_sem=get.at[k],
            device_id=((z + k) % n, y), device_id_type=MESH)

    for k in range(1, n):
        across(stat, stat_send, stat_recv, k, z).start()

    w_copy(0).wait()
    for tile in range(1, tiles):
        w_copy(tile).start()
    acc[0] = jnp.dot(cen[...], w_s[0], preferred_element_type=jnp.float32).astype(jnp.bfloat16)

    def gat_copy(k):
        return pltpu.make_async_remote_copy(
            src_ref=gat.at[0], dst_ref=gat.at[k], send_sem=gat_send.at[k], recv_sem=gat_recv.at[k],
            device_id=(z, partner(y, k, ny)), device_id_type=MESH)

    def z_copy(stage, index, slot, chunk, to):
        return pltpu.make_async_remote_copy(
            src_ref=stg.at[stage, index], dst_ref=recv.at[slot, chunk % slots], send_sem=send_sem.at[stage, index],
            recv_sem=recv_sem.at[slot, chunk % slots], device_id=(to, y), device_id_type=MESH)

    def arrived(slot, chunk):
        pltpu.make_async_remote_copy(
            src_ref=recv.at[slot, chunk % slots], dst_ref=recv.at[slot, chunk % slots], send_sem=send_sem.at[0, 0],
            recv_sem=recv_sem.at[slot, chunk % slots], device_id=((z + 1) % n, y), device_id_type=MESH).wait_recv()

    def landed(slot, chunk):
        return recv[slot, chunk % slots].astype(jnp.float32)

    def rows(plane):
        return pl.ds(pl.multiple_of(plane * part, part), part)

    def forward(chunk, plane, index, out_slot, in_slot, first, to):
        stage = chunk % stages

        @pl.when(chunk >= stages)
        def _():
            z_copy(stage, index, out_slot, chunk, to).wait_send()

        @pl.when(first)
        def _():
            stg[stage, index] = acc[chunk % ring, rows(plane), :]

        @pl.when(jnp.logical_not(first))
        def _():
            arrived(in_slot, chunk)
            stg[stage, index] = (
                acc[chunk % ring, rows(plane), :].astype(jnp.float32) + landed(in_slot, chunk)
            ).astype(jnp.bfloat16)

        z_copy(stage, index, out_slot, chunk, to).start()

    def right_stage(chunk, j):
        forward(chunk, z + 1 + j, j, j, j + 1, z == 0, z + 1)

    def left_stage(chunk, j):
        forward(chunk, z - 1 - j, n - 2 - j, n - j, n - 1 - j, z == n - 1, z - 1)

    @pl.when(z == 0)
    def _():
        for j in reversed(range(n - 1)):
            right_stage(jnp.int32(0), j)

    @pl.when(z == n - 1)
    def _():
        for j in reversed(range(n - 1)):
            left_stage(jnp.int32(0), j)

    for k in range(1, n):
        across(stat, stat_send, stat_recv, k, (z + n - k) % n).wait_recv()
    sums = [stat[k, 0:1, :] for k in range(n)]
    mean = functools.reduce(lambda a, b: a + b, sums) / model
    spread = jnp.zeros_like(mean)
    for k in range(n):
        shift = sums[k] / depth - mean
        spread = spread + stat[k, 1:2, :] + depth * shift * shift
    rstd = lax.rsqrt(spread / model + EPSILON)
    line = lax.broadcasted_iota(jnp.int32, (128, tok), 0)
    table = jnp.where(line == n, rstd, mean)
    for k in range(n):
        table = jnp.where(line == k, (sums[k] / depth - mean) * rstd, table)
    coef[...] = table.T
    gat[0] = (
        (gat[0].astype(jnp.float32) - coef[:, n + 1:n + 2]) * coef[:, n:n + 1] * gain_row()
    ).astype(jnp.bfloat16)
    for k in range(1, ny):
        gat_copy(k).start()

    block = min(part, max(16, 256 // ny))

    def place(chunk, value):
        group, tile = chunk // tiles, chunk % tiles
        row = lax.broadcasted_iota(jnp.int32, (block * ny, block), 0)
        col = lax.broadcasted_iota(jnp.int32, (block * ny, block), 1)
        take = (row == col * ny + partner(y, group, ny)).astype(jnp.bfloat16)
        for b in range(part // block):
            moved = jnp.dot(
                take, value[b * block:(b + 1) * block], preferred_element_type=jnp.float32).astype(jnp.bfloat16)
            span = slice(b * block * ny, (b + 1) * block * ny)

            @pl.when(group == 0)
            def _():
                out_ref[span, cols(tile)] = moved

            @pl.when(group > 0)
            def _():
                out_ref[span, cols(tile)] += moved

    @pl.loop(1, chunks + n - 1)
    def _(it):
        @pl.when(it < chunks)
        def _():
            tile, group = it % tiles, it // tiles

            @pl.when(group == 0)
            def _():
                w_copy(tile).wait()

            @pl.when(jnp.logical_and(group > 0, tile == 0))
            def _():
                gat_copy(group).wait_recv()

            acc[it % ring] = jnp.dot(gat[group], w_s[tile], preferred_element_type=jnp.float32).astype(jnp.bfloat16)

        for j in reversed(range(n - 1)):
            chunk = it - (n - 2 - j)
            inside = jnp.logical_and(chunk >= 0, chunk < chunks)
            later = jnp.logical_and(chunk >= 1, chunk < chunks)

            @pl.when(jnp.logical_and(z + 1 + j < n, jnp.where(z == 0, later, inside)))
            def _():
                right_stage(chunk, j)

            @pl.when(jnp.logical_and(z - 1 - j >= 0, jnp.where(z == n - 1, later, inside)))
            def _():
                left_stage(chunk, j)

        @pl.when(it == 1)
        def _():
            gain = gain_row()
            high = gain.astype(jnp.bfloat16).astype(jnp.float32)
            term = lax.broadcasted_iota(jnp.int32, (16, depth), 0)
            pair = jnp.where(term == 0, high, jnp.where(term == 1, gain - high, 0.0)).astype(jnp.bfloat16)
            both = jnp.dot(pair, w_s[0], preferred_element_type=jnp.float32)
            gw[z] = both[0:1] + both[1:2]
            for k in range(1, n):
                across(gw, gw_send, gw_recv, k, z).start()

        own = it - (n - 1)

        @pl.when(own == 0)
        def _():
            fin[...] = acc[0, rows(z), :].astype(jnp.float32)

            @pl.when(z > 0)
            def _():
                arrived(0, 0)
                fin[...] += landed(0, 0)

            @pl.when(z < n - 1)
            def _():
                arrived(n, 0)
                fin[...] += landed(n, 0)

            for k in range(1, n):
                across(gw, gw_send, gw_recv, k, (z + n - k) % n).wait_recv()
            mine = coef[rows(z), :]
            value = fin[...] * mine[:, n:n + 1]
            for k in range(n):
                value = value + mine[:, k:k + 1] * gw[k]
            fin[...] = value

        @pl.when(own >= 1)
        def _():
            mine = acc[own % ring, rows(z), :].astype(jnp.float32)

            @pl.when(z == 0)
            def _():
                arrived(n, own)
                fin[...] = mine + landed(n, own)

            @pl.when(z == n - 1)
            def _():
                arrived(0, own)
                fin[...] = mine + landed(0, own)

            @pl.when(jnp.logical_and(z > 0, z < n - 1))
            def _():
                arrived(0, own)
                arrived(n, own)
                fin[...] = mine + landed(0, own) + landed(n, own)

        @pl.when(own >= 0)
        def _():
            place(own, fin[...].astype(jnp.bfloat16))

    for chunk in range(chunks - stages, chunks):
        for index in range(n - 1):
            z_copy(chunk % stages, index, 0, chunk, (z + 1) % n).wait_send()
    for k in range(1, n):
        across(stat, stat_send, stat_recv, k, z).wait_send()
        across(gw, gw_send, gw_recv, k, z).wait_send()
    for k in range(1, ny):
        gat_copy(k).wait_send()


def tile_width(columns, most=7):
    if columns % 128:
        return columns
    lanes = columns // 128
    return 128 * max(k for k in range(1, most + 1) if lanes % k == 0)


def solution(mesh):
    n, ny = mesh.shape["gx"], mesh.shape["gy"]

    def body(tokens, norm_gain, joined_weight):
        tok, depth = tokens.shape
        columns = joined_weight.shape[1]
        part, width = tok // n, tile_width(columns)
        tiles = columns // width
        dma = pltpu.SemaphoreType.DMA
        out = pl.pallas_call(
            functools.partial(kernel, n, ny, width),
            out_shape=pltpu.VMEM((part * ny, columns), jnp.bfloat16),
            in_specs=[pl.BlockSpec(memory_space=pl.ANY)] * 3,
            out_specs=pl.BlockSpec(memory_space=pltpu.VMEM),
            scratch_shapes=[
                pltpu.VMEM((tiles, depth, width), jnp.bfloat16),
                pltpu.VMEM((ny, tok, depth), jnp.bfloat16),
                pltpu.VMEM((depth,), jnp.float32),
                pltpu.VMEM((n, 8, tok), jnp.float32),
                pltpu.VMEM((n + 1, n + 1, part, width), jnp.bfloat16),
                pltpu.VMEM((n, tok, width), jnp.bfloat16),
                pltpu.VMEM((STAGES, n - 1, part, width), jnp.bfloat16),
                pltpu.VMEM((tok, depth), jnp.bfloat16),
                pltpu.VMEM((tok, 128), jnp.float32),
                pltpu.VMEM((n + 8, 1, width), jnp.float32),
                pltpu.VMEM((part, width), jnp.float32),
                dma, dma, dma((tiles,)), dma((n,)), dma((n,)), dma((n,)), dma((n,)),
                dma((ny,)), dma((ny,)),
                dma((STAGES, n - 1)), dma((n + 1, n + 1)),
            ],
            compiler_params=pltpu.CompilerParams(
                collective_id=0, has_side_effects=True, vmem_limit_bytes=58 * 2 ** 20),
        )(tokens, norm_gain, joined_weight)
        return out.reshape(part, ny, columns)

    return jax.shard_map(
        body,
        mesh=mesh,
        in_specs=(P("gy", "gx"), P("gx"), P("gx", "gy")),
        out_specs=P("gx", None, "gy"),
        check_vma=False,
    )
```

```python
import functools

import jax
import jax.numpy as jnp
from jax import lax
from jax.experimental import pallas as pl
from jax.experimental.pallas import tpu as pltpu
from jax.sharding import PartitionSpec as P

MESH = pl.DeviceIdType.MESH
EPSILON = 1e-06
STAGES = 4


def partner(y, step, ny):
    out, bit = 0, 1
    while bit < ny:
        out = out + bit * ((y // bit + step // bit) % 2)
        bit *= 2
    return out


def kernel(n, ny, width, tok_ref, gain_hbm, w_hbm, out_ref, w_s, gat, gain_s, stat, recv, acc, stg,
           cen, coef, gw, fin, tok_sem, gain_sem, w_sem, stat_send, stat_recv, gw_send, gw_recv, gat_send, gat_recv,
           send_sem, recv_sem):
    z, y = lax.axis_index("gx"), lax.axis_index("gy")
    tok, depth = tok_ref.shape
    part = tok // n
    stages = stg.shape[0]
    slots = recv.shape[1]
    columns = w_hbm.shape[1]
    tiles = columns // width
    chunks = ny * tiles
    ring = acc.shape[0]
    model = depth * n

    def cols(tile):
        if tiles == 1:
            return slice(None)
        return pl.ds(pl.multiple_of(tile * width, 128), width)

    def w_copy(tile):
        return pltpu.make_async_copy(w_hbm.at[:, cols(tile)], w_s.at[tile], w_sem.at[tile])

    edges = (0, 256, width) if width > 256 else (0, width)
    pieces = [slice(lo, hi) for lo, hi in zip(edges, edges[1:])]

    def w_piece(i):
        return pltpu.make_async_copy(
            w_hbm.at[:, pieces[i]], w_s.at[0, :, pieces[i]], w_sem.at[tiles if i else 0])

    tok_copy = pltpu.make_async_copy(tok_ref, gat.at[0], tok_sem)
    tok_copy.start()
    gain_copy = pltpu.make_async_copy(gain_hbm, gain_s, gain_sem)
    gain_copy.start()
    for i in range(len(pieces)):
        w_piece(i).start()

    barrier = pltpu.get_barrier_semaphore()
    for k in range(1, n):
        pl.semaphore_signal(barrier, inc=1, device_id=((z + k) % n, y), device_id_type=MESH)
    for k in range(1, ny):
        pl.semaphore_signal(barrier, inc=1, device_id=(z, partner(y, k, ny)), device_id_type=MESH)

    def gain_row():
        return gain_s[...].reshape(1, depth)

    tok_copy.wait()
    values = gat[0].astype(jnp.float32)
    total = jnp.sum(values, axis=1, keepdims=True)
    off = values - total / depth
    squares = jnp.sum(off * off, axis=1, keepdims=True)
    lane = lax.broadcasted_iota(jnp.int32, (tok, 128), 1)
    packed = jnp.where(lane == 0, total, squares)
    stat[z] = packed.T[:8]

    gain_copy.wait()
    cen[...] = (off * gain_row()).astype(jnp.bfloat16)

    def across(ref, send, get, k, slot):
        return pltpu.make_async_remote_copy(
            src_ref=ref.at[slot], dst_ref=ref.at[slot], send_sem=send.at[k], recv_sem=get.at[k],
            device_id=((z + k) % n, y), device_id_type=MESH)

    def gat_copy(k):
        return pltpu.make_async_remote_copy(
            src_ref=gat.at[0], dst_ref=gat.at[k], send_sem=gat_send.at[k], recv_sem=gat_recv.at[k],
            device_id=(z, partner(y, k, ny)), device_id_type=MESH)

    def z_copy(stage, index, slot, chunk, to):
        return pltpu.make_async_remote_copy(
            src_ref=stg.at[stage, index], dst_ref=recv.at[slot, chunk % slots], send_sem=send_sem.at[stage, index],
            recv_sem=recv_sem.at[slot, chunk % slots], device_id=(to, y), device_id_type=MESH)

    def arrived(slot, chunk):
        pltpu.make_async_remote_copy(
            src_ref=recv.at[slot, chunk % slots], dst_ref=recv.at[slot, chunk % slots], send_sem=send_sem.at[0, 0],
            recv_sem=recv_sem.at[slot, chunk % slots], device_id=((z + 1) % n, y), device_id_type=MESH).wait_recv()

    def landed(slot, chunk):
        return recv[slot, chunk % slots].astype(jnp.float32)

    def rows(plane):
        return pl.ds(pl.multiple_of(plane * part, part), part)

    def forward(chunk, plane, index, out_slot, in_slot, first, to):
        stage = chunk % stages

        @pl.when(chunk >= stages)
        def _():
            z_copy(stage, index, out_slot, chunk, to).wait_send()

        @pl.when(first)
        def _():
            stg[stage, index] = acc[chunk % ring, rows(plane), :]

        @pl.when(jnp.logical_not(first))
        def _():
            arrived(in_slot, chunk)
            stg[stage, index] = (
                acc[chunk % ring, rows(plane), :].astype(jnp.float32) + landed(in_slot, chunk)
            ).astype(jnp.bfloat16)

        z_copy(stage, index, out_slot, chunk, to).start()

    def right_stage(chunk, j):
        forward(chunk, z + 1 + j, j, j, j + 1, z == 0, z + 1)

    def left_stage(chunk, j):
        forward(chunk, z - 1 - j, n - 2 - j, n - j, n - 1 - j, z == n - 1, z - 1)

    def open_stage(plane, index, slot, piece, to):
        stg[0, index, :, piece] = acc[0, rows(plane), piece]
        pltpu.make_async_remote_copy(
            src_ref=stg.at[0, index, :, piece], dst_ref=recv.at[slot, 0, :, piece], send_sem=send_sem.at[0, index],
            recv_sem=recv_sem.at[slot, 0], device_id=(to, y), device_id_type=MESH).start()

    for i, piece in enumerate(pieces):
        w_piece(i).wait()
        if i == len(pieces) - 1:
            for tile in range(1, tiles):
                w_copy(tile).start()
        acc[0, :, piece] = jnp.dot(
            cen[...], w_s[0, :, piece], preferred_element_type=jnp.float32).astype(jnp.bfloat16)
        if i == 0:
            pl.semaphore_wait(barrier, n - 1 + ny - 1)

        @pl.when(z == 0)
        def _():
            for j in reversed(range(n - 1)):
                open_stage(1 + j, j, j, piece, 1)

        @pl.when(z == n - 1)
        def _():
            for j in reversed(range(n - 1)):
                open_stage(n - 2 - j, n - 2 - j, n - j, piece, n - 2)

        if i == 0:
            for k in range(1, n):
                across(stat, stat_send, stat_recv, k, z).start()

    for k in range(1, n):
        across(stat, stat_send, stat_recv, k, (z + n - k) % n).wait_recv()
    sums = [stat[k, 0:1, :] for k in range(n)]
    mean = functools.reduce(lambda a, b: a + b, sums) / model
    spread = jnp.zeros_like(mean)
    for k in range(n):
        shift = sums[k] / depth - mean
        spread = spread + stat[k, 1:2, :] + depth * shift * shift
    rstd = lax.rsqrt(spread / model + EPSILON)
    line = lax.broadcasted_iota(jnp.int32, (128, tok), 0)
    table = jnp.where(line == n, rstd, mean)
    for k in range(n):
        table = jnp.where(line == k, (sums[k] / depth - mean) * rstd, table)
    coef[...] = table.T
    gat[0] = (
        (gat[0].astype(jnp.float32) - coef[:, n + 1:n + 2]) * coef[:, n:n + 1] * gain_row()
    ).astype(jnp.bfloat16)
    for k in range(1, ny):
        gat_copy(k).start()

    block = min(part, max(16, 256 // ny))

    def place(chunk, value):
        group, tile = chunk // tiles, chunk % tiles
        row = lax.broadcasted_iota(jnp.int32, (block * ny, block), 0)
        col = lax.broadcasted_iota(jnp.int32, (block * ny, block), 1)
        take = (row == col * ny + partner(y, group, ny)).astype(jnp.bfloat16)
        for b in range(part // block):
            moved = jnp.dot(
                take, value[b * block:(b + 1) * block], preferred_element_type=jnp.float32).astype(jnp.bfloat16)
            span = slice(b * block * ny, (b + 1) * block * ny)

            @pl.when(group == 0)
            def _():
                out_ref[span, cols(tile)] = moved

            @pl.when(group > 0)
            def _():
                out_ref[span, cols(tile)] += moved

    @pl.loop(1, chunks + n - 1)
    def _(it):
        @pl.when(it < chunks)
        def _():
            tile, group = it % tiles, it // tiles

            @pl.when(group == 0)
            def _():
                w_copy(tile).wait()

            @pl.when(jnp.logical_and(group > 0, tile == 0))
            def _():
                gat_copy(group).wait_recv()

            acc[it % ring] = jnp.dot(gat[group], w_s[tile], preferred_element_type=jnp.float32).astype(jnp.bfloat16)

        for j in reversed(range(n - 1)):
            chunk = it - (n - 2 - j)
            inside = jnp.logical_and(chunk >= 0, chunk < chunks)
            later = jnp.logical_and(chunk >= 1, chunk < chunks)

            left = jnp.logical_and(z - 1 - j >= 0, jnp.where(z == n - 1, later, inside))

            @pl.when(jnp.logical_and(left, 2 * z < n))
            def _():
                left_stage(chunk, j)

            @pl.when(jnp.logical_and(z + 1 + j < n, jnp.where(z == 0, later, inside)))
            def _():
                right_stage(chunk, j)

            @pl.when(jnp.logical_and(left, 2 * z >= n))
            def _():
                left_stage(chunk, j)

        @pl.when(it == 1)
        def _():
            gain = gain_row()
            high = gain.astype(jnp.bfloat16).astype(jnp.float32)
            term = lax.broadcasted_iota(jnp.int32, (16, depth), 0)
            pair = jnp.where(term == 0, high, jnp.where(term == 1, gain - high, 0.0)).astype(jnp.bfloat16)
            both = jnp.dot(pair, w_s[0], preferred_element_type=jnp.float32)
            gw[z] = both[0:1] + both[1:2]
            for k in range(1, n):
                across(gw, gw_send, gw_recv, k, z).start()

        own = it - (n - 1)

        @pl.when(own == 0)
        def _():
            fin[...] = acc[0, rows(z), :].astype(jnp.float32)

            @pl.when(z > 0)
            def _():
                arrived(0, 0)
                fin[...] += landed(0, 0)

            @pl.when(z < n - 1)
            def _():
                arrived(n, 0)
                fin[...] += landed(n, 0)

            for k in range(1, n):
                across(gw, gw_send, gw_recv, k, (z + n - k) % n).wait_recv()
            mine = coef[rows(z), :]
            value = fin[...] * mine[:, n:n + 1]
            for k in range(n):
                value = value + mine[:, k:k + 1] * gw[k]
            fin[...] = value

        @pl.when(own >= 1)
        def _():
            mine = acc[own % ring, rows(z), :].astype(jnp.float32)

            @pl.when(z == 0)
            def _():
                arrived(n, own)
                fin[...] = mine + landed(n, own)

            @pl.when(z == n - 1)
            def _():
                arrived(0, own)
                fin[...] = mine + landed(0, own)

            @pl.when(jnp.logical_and(z > 0, z < n - 1))
            def _():
                arrived(0, own)
                arrived(n, own)
                fin[...] = mine + landed(0, own) + landed(n, own)

        @pl.when(own >= 0)
        def _():
            place(own, fin[...].astype(jnp.bfloat16))

    for chunk in range(chunks - stages, chunks):
        for index in range(n - 1):
            z_copy(chunk % stages, index, 0, chunk, (z + 1) % n).wait_send()
    for k in range(1, n):
        across(stat, stat_send, stat_recv, k, z).wait_send()
        across(gw, gw_send, gw_recv, k, z).wait_send()
    for k in range(1, ny):
        gat_copy(k).wait_send()


def tile_width(columns, most=7):
    if columns % 128:
        return columns
    lanes = columns // 128
    return 128 * max(k for k in range(1, most + 1) if lanes % k == 0)


def solution(mesh):
    n, ny = mesh.shape["gx"], mesh.shape["gy"]

    def body(tokens, norm_gain, joined_weight):
        tok, depth = tokens.shape
        columns = joined_weight.shape[1]
        part, width = tok // n, tile_width(columns)
        tiles = columns // width
        dma = pltpu.SemaphoreType.DMA
        out = pl.pallas_call(
            functools.partial(kernel, n, ny, width),
            out_shape=pltpu.VMEM((part * ny, columns), jnp.bfloat16),
            in_specs=[pl.BlockSpec(memory_space=pl.ANY)] * 3,
            out_specs=pl.BlockSpec(memory_space=pltpu.VMEM),
            scratch_shapes=[
                pltpu.VMEM((tiles, depth, width), jnp.bfloat16),
                pltpu.VMEM((ny, tok, depth), jnp.bfloat16),
                pltpu.VMEM((depth,), jnp.float32),
                pltpu.VMEM((n, 8, tok), jnp.float32),
                pltpu.VMEM((n + 1, n + 1, part, width), jnp.bfloat16),
                pltpu.VMEM((n, tok, width), jnp.bfloat16),
                pltpu.VMEM((STAGES, n - 1, part, width), jnp.bfloat16),
                pltpu.VMEM((tok, depth), jnp.bfloat16),
                pltpu.VMEM((tok, 128), jnp.float32),
                pltpu.VMEM((n + 8, 1, width), jnp.float32),
                pltpu.VMEM((part, width), jnp.float32),
                dma, dma, dma((tiles + 1,)), dma((n,)), dma((n,)), dma((n,)), dma((n,)),
                dma((ny,)), dma((ny,)),
                dma((STAGES, n - 1)), dma((n + 1, n + 1)),
            ],
            compiler_params=pltpu.CompilerParams(
                collective_id=0, has_side_effects=True, vmem_limit_bytes=58 * 2 ** 20),
        )(tokens, norm_gain, joined_weight)
        return out.reshape(part, ny, columns)

    return jax.shard_map(
        body,
        mesh=mesh,
        in_specs=(P("gy", "gx"), P("gx"), P("gx", "gy")),
        out_specs=P("gx", None, "gy"),
        check_vma=False,
    )
```

```python
import functools

import jax
import jax.numpy as jnp
from jax import lax
from jax.experimental import pallas as pl
from jax.experimental.pallas import tpu as pltpu
from jax.sharding import PartitionSpec as P

MESH = pl.DeviceIdType.MESH
EPSILON = 1e-06
STAGES = 4
EARLY = 2


def partner(y, step, ny):
    out, bit = 0, 1
    while bit < ny:
        out = out + bit * ((y // bit + step // bit) % 2)
        bit *= 2
    return out


def kernel(n, ny, width, tok_ref, gain_hbm, w_hbm, out_ref, w_s, gat, gain_s, stat, recv, acc, stg,
           cen, coef, gw, fin, tok_sem, gain_sem, w_sem, stat_send, stat_recv, gw_send, gw_recv, gat_send, gat_recv,
           send_sem, recv_sem, met):
    z, y = lax.axis_index("gx"), lax.axis_index("gy")
    tok, depth = tok_ref.shape
    part = tok // n
    stages = stg.shape[0]
    slots = recv.shape[1]
    columns = w_hbm.shape[1]
    tiles = columns // width
    chunks = ny * tiles
    ring = acc.shape[0]
    model = depth * n

    def cols(tile, piece=slice(0, width)):
        if tiles == 1:
            return piece
        return pl.ds(pl.multiple_of(tile * width + piece.start, 128), piece.stop - piece.start)

    def w_copy(tile):
        return pltpu.make_async_copy(w_hbm.at[:, cols(tile)], w_s.at[tile], w_sem.at[tile])

    edges = (0, 384, width) if width > 384 else (0, width)
    pieces = [slice(lo, hi) for lo, hi in zip(edges, edges[1:])]

    def w_piece(i):
        return pltpu.make_async_copy(
            w_hbm.at[:, pieces[i]], w_s.at[0, :, pieces[i]], w_sem.at[tiles if i else 0])

    def rows(plane):
        return pl.ds(pl.multiple_of(plane * part, part), part)

    order = [jnp.where(2 * z < n, n - 1 - i, i) for i in range(n)]

    def tok_copy(i):
        return pltpu.make_async_copy(tok_ref.at[rows(order[i])], gat.at[0, rows(order[i])], tok_sem.at[i])

    for i in range(n):
        tok_copy(i).start()
    gain_copy = pltpu.make_async_copy(gain_hbm, gain_s, gain_sem)
    gain_copy.start()
    for i in range(len(pieces)):
        w_piece(i).start()

    bits = (ny - 1).bit_length()
    degree = (z > 0).astype(jnp.int32) + (z < n - 1).astype(jnp.int32) + bits

    def greet(sem):
        @pl.when(z > 0)
        def _():
            pl.semaphore_signal(sem, inc=1, device_id=(z - 1, y), device_id_type=MESH)

        @pl.when(z < n - 1)
        def _():
            pl.semaphore_signal(sem, inc=1, device_id=(z + 1, y), device_id_type=MESH)

        for bit in range(bits):
            pl.semaphore_signal(sem, inc=1, device_id=(z, partner(y, 1 << bit, ny)), device_id_type=MESH)

    barrier = pltpu.get_barrier_semaphore()
    greet(barrier)

    def gain_row():
        return gain_s[...].reshape(1, depth)

    def across(ref, send, get, k, slot):
        return pltpu.make_async_remote_copy(
            src_ref=ref.at[slot], dst_ref=ref.at[slot], send_sem=send.at[k], recv_sem=get.at[k],
            device_id=((z + k) % n, y), device_id_type=MESH)

    def gat_copy(k):
        return pltpu.make_async_remote_copy(
            src_ref=gat.at[0], dst_ref=gat.at[k], send_sem=gat_send.at[k], recv_sem=gat_recv.at[k],
            device_id=(z, partner(y, k, ny)), device_id_type=MESH)

    def z_copy(stage, index, slot, chunk, to):
        return pltpu.make_async_remote_copy(
            src_ref=stg.at[stage, index], dst_ref=recv.at[slot, chunk % slots], send_sem=send_sem.at[stage, index],
            recv_sem=recv_sem.at[slot, chunk % slots], device_id=(to, y), device_id_type=MESH)

    last = chunks - 1
    cut = (width - 256) // 128 * 128
    ends = [slice(0, cut), slice(cut, width)] if cut > 0 else [slice(0, width)]

    def end_copy(index, slot, i, to):
        return pltpu.make_async_remote_copy(
            src_ref=stg.at[last % stages, index, :, ends[i]], dst_ref=recv.at[slot, last % slots, :, ends[i]],
            send_sem=send_sem.at[last % stages, index], recv_sem=recv_sem.at[slot, slots if i else last % slots],
            device_id=(to, y), device_id_type=MESH)

    def arrived(slot, chunk):
        pltpu.make_async_remote_copy(
            src_ref=recv.at[slot, chunk % slots], dst_ref=recv.at[slot, chunk % slots], send_sem=send_sem.at[0, 0],
            recv_sem=recv_sem.at[slot, chunk % slots], device_id=((z + 1) % n, y), device_id_type=MESH).wait_recv()

    def landed(slot, chunk):
        return recv[slot, chunk % slots].astype(jnp.float32)

    def forward(chunk, plane, index, out_slot, in_slot, first, to, whole):
        stage = chunk % stages

        @pl.when(chunk >= stages)
        def _():
            z_copy(stage, index, out_slot, chunk, to).wait_send()

        @pl.when(first)
        def _():
            stg[stage, index] = acc[chunk % ring, rows(plane), :]

        @pl.when(jnp.logical_not(first))
        def _():
            arrived(in_slot, chunk)
            stg[stage, index] = (
                acc[chunk % ring, rows(plane), :].astype(jnp.float32) + landed(in_slot, chunk)
            ).astype(jnp.bfloat16)

        if whole:
            z_copy(stage, index, out_slot, chunk, to).start()
        else:
            for i in range(len(ends)):
                end_copy(index, out_slot, i, to).start()

    def right_stage(chunk, j, whole=True):
        forward(chunk, z + 1 + j, j, j, j + 1, z == 0, z + 1, whole)

    def left_stage(chunk, j, whole=True):
        forward(chunk, z - 1 - j, n - 2 - j, n - j, n - 1 - j, z == n - 1, z - 1, whole)

    def open_stage(plane, index, slot, piece, to):
        stg[0, index, :, piece] = acc[0, rows(plane), piece]
        pltpu.make_async_remote_copy(
            src_ref=stg.at[0, index, :, piece], dst_ref=recv.at[slot, 0, :, piece], send_sem=send_sem.at[0, index],
            recv_sem=recv_sem.at[slot, 0], device_id=(to, y), device_id_type=MESH).start()

    gain_copy.wait()
    lane = lax.broadcasted_iota(jnp.int32, (part, 128), 1)
    for i in range(n):
        mine = rows(order[i])
        tok_copy(i).wait()
        values = gat[0, mine, :].astype(jnp.float32)
        total = jnp.sum(values, axis=1, keepdims=True)
        off = values - total / depth
        squares = jnp.sum(off * off, axis=1, keepdims=True)
        coef[mine, :] = jnp.where(lane == 0, total, squares)
        cen[mine, :] = (off * gain_row()).astype(jnp.bfloat16)
        if i == 0:
            w_piece(0).wait()
        acc[0, mine, pieces[0]] = jnp.dot(
            cen[mine, :], w_s[0, :, pieces[0]], preferred_element_type=jnp.float32).astype(jnp.bfloat16)
        if i == 0:
            pl.semaphore_wait(barrier, degree)
            greet(met.at[0])
        if i < n - 1:
            @pl.when(z == 0)
            def _():
                open_stage(n - 1 - i, n - 2 - i, n - 2 - i, pieces[0], 1)

            @pl.when(z == n - 1)
            def _():
                open_stage(i, i, i + 2, pieces[0], n - 2)

    def near(k):
        return jnp.abs((z + k) % n - z) == 1

    stat[z] = coef[...].T[:8]
    for k in range(1, n):
        @pl.when(near(k))
        def _():
            across(stat, stat_send, stat_recv, k, z).start()

    rounds = met.shape[0]
    for r in range(1, rounds):
        pl.semaphore_wait(met.at[r - 1], degree)
        greet(met.at[r])

    if len(pieces) > 1:
        w_piece(1).wait()
    for tile in range(1, tiles):
        w_copy(tile).start()
    for piece in pieces[1:]:
        acc[0, :, piece] = jnp.dot(
            cen[...], w_s[0, :, piece], preferred_element_type=jnp.float32).astype(jnp.bfloat16)

        @pl.when(z == 0)
        def _():
            for j in reversed(range(n - 1)):
                open_stage(1 + j, j, j, piece, 1)

        @pl.when(z == n - 1)
        def _():
            for j in reversed(range(n - 1)):
                open_stage(n - 2 - j, n - 2 - j, n - j, piece, n - 2)

    pl.semaphore_wait(met.at[rounds - 1], degree)
    for k in range(1, n):
        @pl.when(jnp.logical_not(near(k)))
        def _():
            across(stat, stat_send, stat_recv, k, z).start()

    early = min(EARLY, tiles)
    gain = gain_row()
    high = gain.astype(jnp.bfloat16).astype(jnp.float32)
    term = lax.broadcasted_iota(jnp.int32, (16, depth), 0)
    pair = jnp.where(term == 0, high, jnp.where(term == 1, gain - high, 0.0)).astype(jnp.bfloat16)
    for tile in range(early):
        if tile > 0:
            w_copy(tile).wait()
        both = jnp.dot(pair, w_s[tile], preferred_element_type=jnp.float32)
        gw[z, :, tile * width:(tile + 1) * width] = both[0:1] + both[1:2]
    for k in range(1, n):
        across(gw, gw_send, gw_recv, k, z).start()

    for tile in range(1, early):
        acc[tile] = jnp.dot(cen[...], w_s[tile], preferred_element_type=jnp.float32).astype(jnp.bfloat16)

        @pl.when(z == 0)
        def _():
            for j in reversed(range(n - 1)):
                right_stage(jnp.int32(tile), j)

        @pl.when(z == n - 1)
        def _():
            for j in reversed(range(n - 1)):
                left_stage(jnp.int32(tile), j)

    for k in range(1, n):
        across(stat, stat_send, stat_recv, k, (z + n - k) % n).wait_recv()
    sums = [stat[k, 0:1, :] for k in range(n)]
    mean = functools.reduce(lambda a, b: a + b, sums) / model
    spread = jnp.zeros_like(mean)
    for k in range(n):
        shift = sums[k] / depth - mean
        spread = spread + stat[k, 1:2, :] + depth * shift * shift
    rstd = lax.rsqrt(spread / model + EPSILON)
    line = lax.broadcasted_iota(jnp.int32, (128, tok), 0)
    table = jnp.where(line == n, rstd, mean)
    for k in range(n):
        table = jnp.where(line == k, (sums[k] / depth - mean) * rstd, table)
    coef[...] = table.T
    gat[0] = (
        (gat[0].astype(jnp.float32) - coef[:, n + 1:n + 2]) * coef[:, n:n + 1] * gain_row()
    ).astype(jnp.bfloat16)
    for k in range(1, ny):
        gat_copy(k).start()

    block = min(part, max(16, 256 // ny))

    def place(chunk, value, piece=slice(0, width)):
        group, tile = chunk // tiles, chunk % tiles
        row = lax.broadcasted_iota(jnp.int32, (block * ny, block), 0)
        col = lax.broadcasted_iota(jnp.int32, (block * ny, block), 1)
        take = (row == col * ny + partner(y, group, ny)).astype(jnp.bfloat16)
        for b in range(part // block):
            moved = jnp.dot(
                take, value[b * block:(b + 1) * block], preferred_element_type=jnp.float32).astype(jnp.bfloat16)
            span = slice(b * block * ny, (b + 1) * block * ny)

            @pl.when(group == 0)
            def _():
                out_ref[span, cols(tile, piece)] = moved

            @pl.when(group > 0)
            def _():
                out_ref[span, cols(tile, piece)] += moved

    def settle(chunk, wait, piece=slice(0, width)):
        mine = acc[chunk % ring, rows(z), piece].astype(jnp.float32)

        def there(slot):
            return recv[slot, chunk % slots, :, piece].astype(jnp.float32)

        @pl.when(z == 0)
        def _():
            wait(n)
            fin[:, piece] = mine + there(n)

        @pl.when(z == n - 1)
        def _():
            wait(0)
            fin[:, piece] = mine + there(0)

        @pl.when(jnp.logical_and(z > 0, z < n - 1))
        def _():
            wait(0)
            wait(n)
            fin[:, piece] = mine + there(0) + there(n)

    @pl.loop(1, chunks + n - 3)
    def _(it):
        @pl.when(jnp.logical_and(it >= early, it < chunks))
        def _():
            tile, group = it % tiles, it // tiles

            @pl.when(group == 0)
            def _():
                w_copy(tile).wait()

            @pl.when(jnp.logical_and(group > 0, tile == 0))
            def _():
                gat_copy(group).wait_recv()

            acc[it % ring] = jnp.dot(gat[group], w_s[tile], preferred_element_type=jnp.float32).astype(jnp.bfloat16)

        for j in reversed(range(n - 1)):
            chunk = it - (n - 2 - j)
            inside = jnp.logical_and(chunk >= 0, chunk < chunks)
            later = jnp.logical_and(chunk >= early, chunk < chunks)

            left = jnp.logical_and(z - 1 - j >= 0, jnp.where(z == n - 1, later, inside))

            @pl.when(jnp.logical_and(left, 2 * z < n))
            def _():
                left_stage(chunk, j)

            @pl.when(jnp.logical_and(z + 1 + j < n, jnp.where(z == 0, later, inside)))
            def _():
                right_stage(chunk, j)

            @pl.when(jnp.logical_and(left, 2 * z >= n))
            def _():
                left_stage(chunk, j)

        own = it - (n - 1)

        @pl.when(own >= 0)
        def _():
            settle(own, lambda slot: arrived(slot, own))

        for tile in range(early):
            @pl.when(own == tile)
            def _():
                if tile == 0:
                    for k in range(1, n):
                        across(gw, gw_send, gw_recv, k, (z + n - k) % n).wait_recv()
                mine = coef[rows(z), :]
                value = fin[...] * mine[:, n:n + 1]
                for k in range(n):
                    value = value + mine[:, k:k + 1] * gw[k, :, tile * width:(tile + 1) * width]
                fin[...] = value

        @pl.when(own >= 0)
        def _():
            place(own, fin[...].astype(jnp.bfloat16))

    @pl.when(jnp.logical_and(z > 0, 2 * z < n))
    def _():
        left_stage(last, 0, False)

    @pl.when(z < n - 1)
    def _():
        right_stage(last, 0, False)

    @pl.when(2 * z >= n)
    def _():
        left_stage(last, 0, False)

    settle(last - 1, lambda slot: arrived(slot, last - 1))
    place(last - 1, fin[...].astype(jnp.bfloat16))
    for i, piece in enumerate(ends):
        settle(last, lambda slot: end_copy(0, slot, i, (z + 1) % n).wait_recv(), piece)
        place(last, fin[:, piece].astype(jnp.bfloat16), piece)

    for chunk in range(chunks - stages, chunks):
        for index in range(n - 1):
            z_copy(chunk % stages, index, 0, chunk, (z + 1) % n).wait_send()
    for k in range(1, n):
        across(stat, stat_send, stat_recv, k, z).wait_send()
        across(gw, gw_send, gw_recv, k, z).wait_send()
    for k in range(1, ny):
        gat_copy(k).wait_send()


def tile_width(columns, most=7):
    if columns % 128:
        return columns
    lanes = columns // 128
    return 128 * max(k for k in range(1, most + 1) if lanes % k == 0)


def solution(mesh):
    n, ny = mesh.shape["gx"], mesh.shape["gy"]

    def body(tokens, norm_gain, joined_weight):
        tok, depth = tokens.shape
        columns = joined_weight.shape[1]
        part, width = tok // n, tile_width(columns)
        tiles = columns // width
        dma = pltpu.SemaphoreType.DMA
        out = pl.pallas_call(
            functools.partial(kernel, n, ny, width),
            out_shape=pltpu.VMEM((part * ny, columns), jnp.bfloat16),
            in_specs=[pl.BlockSpec(memory_space=pl.ANY)] * 3,
            out_specs=pl.BlockSpec(memory_space=pltpu.VMEM),
            scratch_shapes=[
                pltpu.VMEM((tiles, depth, width), jnp.bfloat16),
                pltpu.VMEM((ny, tok, depth), jnp.bfloat16),
                pltpu.VMEM((depth,), jnp.float32),
                pltpu.VMEM((n, 8, tok), jnp.float32),
                pltpu.VMEM((n + 1, n + 1, part, width), jnp.bfloat16),
                pltpu.VMEM((n, tok, width), jnp.bfloat16),
                pltpu.VMEM((STAGES, n - 1, part, width), jnp.bfloat16),
                pltpu.VMEM((tok, depth), jnp.bfloat16),
                pltpu.VMEM((tok, 128), jnp.float32),
                pltpu.VMEM((n + 8, 1, min(EARLY, tiles) * width), jnp.float32),
                pltpu.VMEM((part, width), jnp.float32),
                dma((n,)), dma, dma((tiles + 1,)), dma((n,)), dma((n,)), dma((n,)), dma((n,)),
                dma((ny,)), dma((ny,)),
                dma((STAGES, n - 1)), dma((n + 1, n + 2)),
                pltpu.SemaphoreType.REGULAR((max(n - 1, (ny - 1).bit_length()) - 1,)),
            ],
            compiler_params=pltpu.CompilerParams(
                collective_id=0, has_side_effects=True, vmem_limit_bytes=58 * 2 ** 20),
        )(tokens, norm_gain, joined_weight)
        return out.reshape(part, ny, columns)

    return jax.shard_map(
        body,
        mesh=mesh,
        in_specs=(P("gy", "gx"), P("gx"), P("gx", "gy")),
        out_specs=P("gx", None, "gy"),
        check_vma=False,
    )
```

```python
import functools

import jax
import jax.numpy as jnp
from jax import lax
from jax.experimental import pallas as pl
from jax.experimental.pallas import tpu as pltpu
from jax.sharding import PartitionSpec as P

MESH = pl.DeviceIdType.MESH
EPSILON = 1e-06
STAGES = 4
EARLY = 2


def partner(y, step, ny):
    out, bit = 0, 1
    while bit < ny:
        out = out + bit * ((y // bit + step // bit) % 2)
        bit *= 2
    return out


def kernel(n, ny, width, tok_ref, gain_hbm, w_hbm, out_ref, w_s, gat, gain_s, stat, recv, acc, stg,
           cen, coef, gw, fin, tok_sem, gain_sem, w_sem, stat_send, stat_recv, gw_send, gw_recv, gat_send, gat_recv,
           send_sem, recv_sem, met):
    z, y = lax.axis_index("gx"), lax.axis_index("gy")
    tok, depth = tok_ref.shape
    part = tok // n
    stages = stg.shape[0]
    slots = recv.shape[1]
    columns = w_hbm.shape[1]
    tiles = columns // width
    chunks = ny * tiles
    ring = acc.shape[0]
    model = depth * n

    def cols(tile, piece=slice(0, width)):
        if tiles == 1:
            return piece
        return pl.ds(pl.multiple_of(tile * width + piece.start, 128), piece.stop - piece.start)

    def w_copy(tile):
        return pltpu.make_async_copy(w_hbm.at[:, cols(tile)], w_s.at[tile], w_sem.at[tile])

    edges = (0, 384, width) if width > 384 else (0, width)
    pieces = [slice(lo, hi) for lo, hi in zip(edges, edges[1:])]

    def w_piece(i):
        return pltpu.make_async_copy(
            w_hbm.at[:, pieces[i]], w_s.at[0, :, pieces[i]], w_sem.at[tiles if i else 0])

    def rows(plane):
        return pl.ds(pl.multiple_of(plane * part, part), part)

    order = [jnp.where(2 * z < n, n - 1 - i, i) for i in range(n)]

    def tok_copy(i):
        return pltpu.make_async_copy(tok_ref.at[rows(order[i])], gat.at[0, rows(order[i])], tok_sem.at[i])

    for i in range(n):
        tok_copy(i).start()
    gain_copy = pltpu.make_async_copy(gain_hbm, gain_s, gain_sem)
    gain_copy.start()
    w_piece(0).start()

    bits = (ny - 1).bit_length()
    degree = (z > 0).astype(jnp.int32) + (z < n - 1).astype(jnp.int32) + bits

    def greet(sem):
        @pl.when(z > 0)
        def _():
            pl.semaphore_signal(sem, inc=1, device_id=(z - 1, y), device_id_type=MESH)

        @pl.when(z < n - 1)
        def _():
            pl.semaphore_signal(sem, inc=1, device_id=(z + 1, y), device_id_type=MESH)

        for bit in range(bits):
            pl.semaphore_signal(sem, inc=1, device_id=(z, partner(y, 1 << bit, ny)), device_id_type=MESH)

    barrier = pltpu.get_barrier_semaphore()
    greet(barrier)

    def gain_row():
        return gain_s[...].reshape(1, depth)

    def across(ref, send, get, k, slot):
        return pltpu.make_async_remote_copy(
            src_ref=ref.at[slot], dst_ref=ref.at[slot], send_sem=send.at[k], recv_sem=get.at[k],
            device_id=((z + k) % n, y), device_id_type=MESH)

    def gat_copy(k):
        return pltpu.make_async_remote_copy(
            src_ref=gat.at[0], dst_ref=gat.at[k], send_sem=gat_send.at[k], recv_sem=gat_recv.at[k],
            device_id=(z, partner(y, k, ny)), device_id_type=MESH)

    def z_copy(stage, index, slot, chunk, to):
        return pltpu.make_async_remote_copy(
            src_ref=stg.at[stage, index], dst_ref=recv.at[slot, chunk % slots], send_sem=send_sem.at[stage, index],
            recv_sem=recv_sem.at[slot, chunk % slots], device_id=(to, y), device_id_type=MESH)

    last = chunks - 1
    cut = (width - 256) // 128 * 128
    ends = [slice(0, cut), slice(cut, width)] if cut > 0 else [slice(0, width)]

    def end_copy(index, slot, i, to):
        return pltpu.make_async_remote_copy(
            src_ref=stg.at[last % stages, index, :, ends[i]], dst_ref=recv.at[slot, last % slots, :, ends[i]],
            send_sem=send_sem.at[last % stages, index], recv_sem=recv_sem.at[slot, slots if i else last % slots],
            device_id=(to, y), device_id_type=MESH)

    def arrived(slot, chunk):
        pltpu.make_async_remote_copy(
            src_ref=recv.at[slot, chunk % slots], dst_ref=recv.at[slot, chunk % slots], send_sem=send_sem.at[0, 0],
            recv_sem=recv_sem.at[slot, chunk % slots], device_id=((z + 1) % n, y), device_id_type=MESH).wait_recv()

    def landed(slot, chunk):
        return recv[slot, chunk % slots].astype(jnp.float32)

    def forward(chunk, plane, index, out_slot, in_slot, first, to, whole):
        stage = chunk % stages

        @pl.when(chunk >= stages)
        def _():
            z_copy(stage, index, out_slot, chunk, to).wait_send()

        @pl.when(first)
        def _():
            stg[stage, index] = acc[chunk % ring, rows(plane), :]

        @pl.when(jnp.logical_not(first))
        def _():
            arrived(in_slot, chunk)
            stg[stage, index] = (
                acc[chunk % ring, rows(plane), :].astype(jnp.float32) + landed(in_slot, chunk)
            ).astype(jnp.bfloat16)

        if whole:
            z_copy(stage, index, out_slot, chunk, to).start()
        else:
            for i in range(len(ends)):
                end_copy(index, out_slot, i, to).start()

    def right_stage(chunk, j, whole=True):
        forward(chunk, z + 1 + j, j, j, j + 1, z == 0, z + 1, whole)

    def left_stage(chunk, j, whole=True):
        forward(chunk, z - 1 - j, n - 2 - j, n - j, n - 1 - j, z == n - 1, z - 1, whole)

    def open_stage(plane, index, slot, piece, to):
        stg[0, index, :, piece] = acc[0, rows(plane), piece]
        pltpu.make_async_remote_copy(
            src_ref=stg.at[0, index, :, piece], dst_ref=recv.at[slot, 0, :, piece], send_sem=send_sem.at[0, index],
            recv_sem=recv_sem.at[slot, 0], device_id=(to, y), device_id_type=MESH).start()

    gain_copy.wait()
    lane = lax.broadcasted_iota(jnp.int32, (part, 128), 1)
    for i in range(n):
        mine = rows(order[i])
        tok_copy(i).wait()
        if i == 0 and len(pieces) > 1:
            w_piece(1).start()
        values = gat[0, mine, :].astype(jnp.float32)
        total = jnp.sum(values, axis=1, keepdims=True)
        off = values - total / depth
        squares = jnp.sum(off * off, axis=1, keepdims=True)
        coef[mine, :] = jnp.where(lane == 0, total, squares)
        cen[mine, :] = (off * gain_row()).astype(jnp.bfloat16)
        if i == 0:
            w_piece(0).wait()
        acc[0, mine, pieces[0]] = jnp.dot(
            cen[mine, :], w_s[0, :, pieces[0]], preferred_element_type=jnp.float32).astype(jnp.bfloat16)
        if i == 0:
            pl.semaphore_wait(barrier, degree)
            greet(met.at[0])
        if i < n - 1:
            @pl.when(z == 0)
            def _():
                open_stage(n - 1 - i, n - 2 - i, n - 2 - i, pieces[0], 1)

            @pl.when(z == n - 1)
            def _():
                open_stage(i, i, i + 2, pieces[0], n - 2)

    def near(k):
        return jnp.abs((z + k) % n - z) == 1

    stat[z] = coef[...].T[:2]
    for k in range(1, n):
        @pl.when(near(k))
        def _():
            across(stat, stat_send, stat_recv, k, z).start()

    rounds = met.shape[0]
    for r in range(1, rounds):
        pl.semaphore_wait(met.at[r - 1], degree)
        greet(met.at[r])

    if len(pieces) > 1:
        w_piece(1).wait()
    for tile in range(1, tiles):
        w_copy(tile).start()
    for piece in pieces[1:]:
        acc[0, :, piece] = jnp.dot(
            cen[...], w_s[0, :, piece], preferred_element_type=jnp.float32).astype(jnp.bfloat16)

        @pl.when(z == 0)
        def _():
            for j in reversed(range(n - 1)):
                open_stage(1 + j, j, j, piece, 1)

        @pl.when(z == n - 1)
        def _():
            for j in reversed(range(n - 1)):
                open_stage(n - 2 - j, n - 2 - j, n - j, piece, n - 2)

    pl.semaphore_wait(met.at[rounds - 1], degree)
    for k in range(1, n):
        @pl.when(jnp.logical_not(near(k)))
        def _():
            across(stat, stat_send, stat_recv, k, z).start()

    early = min(EARLY, tiles)
    gain = gain_row()
    high = gain.astype(jnp.bfloat16).astype(jnp.float32)
    term = lax.broadcasted_iota(jnp.int32, (16, depth), 0)
    pair = jnp.where(term == 0, high, jnp.where(term == 1, gain - high, 0.0)).astype(jnp.bfloat16)
    for tile in range(early):
        if tile > 0:
            w_copy(tile).wait()
        both = jnp.dot(pair, w_s[tile], preferred_element_type=jnp.float32)
        gw[z, :, tile * width:(tile + 1) * width] = both[0:1] + both[1:2]
    def gw_copy(source, side):
        return pltpu.make_async_remote_copy(
            src_ref=gw.at[source], dst_ref=gw.at[source], send_sem=gw_send.at[side, source],
            recv_sem=gw_recv.at[source], device_id=(z + 1 if side else z - 1, y), device_id_type=MESH)

    def to_right(hop):
        return jnp.logical_and(z >= hop, z < n - 1)

    def to_left(hop):
        return jnp.logical_and(z + hop < n, z > 0)

    def hand_on(hop):
        @pl.when(to_right(hop))
        def _():
            if hop > 0:
                gw_copy(z - hop, 1).wait_recv()
            gw_copy(z - hop, 1).start()

        @pl.when(to_left(hop))
        def _():
            if hop > 0:
                gw_copy(z + hop, 0).wait_recv()
            gw_copy(z + hop, 0).start()

    hand_on(0)

    for tile in range(1, early):
        acc[tile] = jnp.dot(cen[...], w_s[tile], preferred_element_type=jnp.float32).astype(jnp.bfloat16)

        @pl.when(z == 0)
        def _():
            for j in reversed(range(n - 1)):
                right_stage(jnp.int32(tile), j)

        @pl.when(z == n - 1)
        def _():
            for j in reversed(range(n - 1)):
                left_stage(jnp.int32(tile), j)

    for k in range(1, n):
        across(stat, stat_send, stat_recv, k, (z + n - k) % n).wait_recv()
    sums = [stat[k, 0:1, :] for k in range(n)]
    mean = functools.reduce(lambda a, b: a + b, sums) / model
    spread = jnp.zeros_like(mean)
    for k in range(n):
        shift = sums[k] / depth - mean
        spread = spread + stat[k, 1:2, :] + depth * shift * shift
    rstd = lax.rsqrt(spread / model + EPSILON)
    line = lax.broadcasted_iota(jnp.int32, (128, tok), 0)
    table = jnp.where(line == n, rstd, mean)
    for k in range(n):
        table = jnp.where(line == k, (sums[k] / depth - mean) * rstd, table)
    coef[...] = table.T
    gat[0] = (
        (gat[0].astype(jnp.float32) - coef[:, n + 1:n + 2]) * coef[:, n:n + 1] * gain_row()
    ).astype(jnp.bfloat16)
    for k in range(1, ny):
        gat_copy(k).start()

    block = min(part, max(16, 256 // ny))

    def place(chunk, value, piece=slice(0, width)):
        group, tile = chunk // tiles, chunk % tiles
        row = lax.broadcasted_iota(jnp.int32, (block * ny, block), 0)
        col = lax.broadcasted_iota(jnp.int32, (block * ny, block), 1)
        take = (row == col * ny + partner(y, group, ny)).astype(jnp.bfloat16)
        for b in range(part // block):
            moved = jnp.dot(
                take, value[b * block:(b + 1) * block], preferred_element_type=jnp.float32).astype(jnp.bfloat16)
            span = slice(b * block * ny, (b + 1) * block * ny)

            @pl.when(group == 0)
            def _():
                out_ref[span, cols(tile, piece)] = moved

            @pl.when(group > 0)
            def _():
                out_ref[span, cols(tile, piece)] += moved

    def settle(chunk, wait, piece=slice(0, width)):
        mine = acc[chunk % ring, rows(z), piece].astype(jnp.float32)

        def there(slot):
            return recv[slot, chunk % slots, :, piece].astype(jnp.float32)

        @pl.when(z == 0)
        def _():
            wait(n)
            fin[:, piece] = mine + there(n)

        @pl.when(z == n - 1)
        def _():
            wait(0)
            fin[:, piece] = mine + there(0)

        @pl.when(jnp.logical_and(z > 0, z < n - 1))
        def _():
            wait(0)
            wait(n)
            fin[:, piece] = mine + there(0) + there(n)

    @pl.loop(1, chunks + n - 3)
    def _(it):
        @pl.when(jnp.logical_and(it >= early, it < chunks))
        def _():
            tile, group = it % tiles, it // tiles

            @pl.when(group == 0)
            def _():
                w_copy(tile).wait()

            @pl.when(jnp.logical_and(group > 0, tile == 0))
            def _():
                gat_copy(group).wait_recv()

            acc[it % ring] = jnp.dot(gat[group], w_s[tile], preferred_element_type=jnp.float32).astype(jnp.bfloat16)

        for j in reversed(range(n - 1)):
            chunk = it - (n - 2 - j)
            inside = jnp.logical_and(chunk >= 0, chunk < chunks)
            later = jnp.logical_and(chunk >= early, chunk < chunks)

            left = jnp.logical_and(z - 1 - j >= 0, jnp.where(z == n - 1, later, inside))

            @pl.when(jnp.logical_and(left, 2 * z < n))
            def _():
                left_stage(chunk, j)

            @pl.when(jnp.logical_and(z + 1 + j < n, jnp.where(z == 0, later, inside)))
            def _():
                right_stage(chunk, j)

            @pl.when(jnp.logical_and(left, 2 * z >= n))
            def _():
                left_stage(chunk, j)

        own = it - (n - 1)

        @pl.when(own >= 0)
        def _():
            settle(own, lambda slot: arrived(slot, own))

        for tile in range(early):
            @pl.when(own == tile)
            def _():
                if tile == 0:
                    @pl.when(z == 0)
                    def _():
                        for k in range(1, n):
                            gw_copy(k, 1).wait_recv()

                    @pl.when(z == n - 1)
                    def _():
                        for k in range(n - 1):
                            gw_copy(k, 0).wait_recv()

                mine = coef[rows(z), :]
                value = fin[...] * mine[:, n:n + 1]
                for k in range(n):
                    value = value + mine[:, k:k + 1] * gw[k, :, tile * width:(tile + 1) * width]
                fin[...] = value

        @pl.when(own >= 0)
        def _():
            place(own, fin[...].astype(jnp.bfloat16))

        for hop in range(1, n - 1):
            @pl.when(it == hop)
            def _():
                hand_on(hop)

    @pl.when(jnp.logical_and(z > 0, 2 * z < n))
    def _():
        left_stage(last, 0, False)

    @pl.when(z < n - 1)
    def _():
        right_stage(last, 0, False)

    @pl.when(2 * z >= n)
    def _():
        left_stage(last, 0, False)

    settle(last - 1, lambda slot: arrived(slot, last - 1))
    place(last - 1, fin[...].astype(jnp.bfloat16))
    for i, piece in enumerate(ends):
        settle(last, lambda slot: end_copy(0, slot, i, (z + 1) % n).wait_recv(), piece)
        place(last, fin[:, piece].astype(jnp.bfloat16), piece)

    for chunk in range(chunks - stages, chunks):
        for index in range(n - 1):
            z_copy(chunk % stages, index, 0, chunk, (z + 1) % n).wait_send()
    for k in range(1, n):
        across(stat, stat_send, stat_recv, k, z).wait_send()
    for hop in range(n - 1):
        @pl.when(to_right(hop))
        def _():
            gw_copy(z - hop, 1).wait_send()

        @pl.when(to_left(hop))
        def _():
            gw_copy(z + hop, 0).wait_send()

    for k in range(1, ny):
        gat_copy(k).wait_send()


def tile_width(columns, most=7):
    if columns % 128:
        return columns
    lanes = columns // 128
    return 128 * max(k for k in range(1, most + 1) if lanes % k == 0)


def solution(mesh):
    n, ny = mesh.shape["gx"], mesh.shape["gy"]

    def body(tokens, norm_gain, joined_weight):
        tok, depth = tokens.shape
        columns = joined_weight.shape[1]
        part, width = tok // n, tile_width(columns)
        tiles = columns // width
        dma = pltpu.SemaphoreType.DMA
        out = pl.pallas_call(
            functools.partial(kernel, n, ny, width),
            out_shape=pltpu.VMEM((part * ny, columns), jnp.bfloat16),
            in_specs=[pl.BlockSpec(memory_space=pl.ANY)] * 3,
            out_specs=pl.BlockSpec(memory_space=pltpu.VMEM),
            scratch_shapes=[
                pltpu.VMEM((tiles, depth, width), jnp.bfloat16),
                pltpu.VMEM((ny, tok, depth), jnp.bfloat16),
                pltpu.VMEM((depth,), jnp.float32),
                pltpu.VMEM((n + 8, 2, tok), jnp.float32),
                pltpu.VMEM((n + 1, n + 1, part, width), jnp.bfloat16),
                pltpu.VMEM((n, tok, width), jnp.bfloat16),
                pltpu.VMEM((STAGES, n - 1, part, width), jnp.bfloat16),
                pltpu.VMEM((tok, depth), jnp.bfloat16),
                pltpu.VMEM((tok, 128), jnp.float32),
                pltpu.VMEM((n + 8, 1, min(EARLY, tiles) * width), jnp.float32),
                pltpu.VMEM((part, width), jnp.float32),
                dma((n,)), dma, dma((tiles + 1,)), dma((n,)), dma((n,)), dma((2, n)), dma((n,)),
                dma((ny,)), dma((ny,)),
                dma((STAGES, n - 1)), dma((n + 1, n + 2)),
                pltpu.SemaphoreType.REGULAR((max(n - 1, (ny - 1).bit_length()) - 1,)),
            ],
            compiler_params=pltpu.CompilerParams(
                collective_id=0, has_side_effects=True, vmem_limit_bytes=58 * 2 ** 20),
        )(tokens, norm_gain, joined_weight)
        return out.reshape(part, ny, columns)

    return jax.shard_map(
        body,
        mesh=mesh,
        in_specs=(P("gy", "gx"), P("gx"), P("gx", "gy")),
        out_specs=P("gx", None, "gy"),
        check_vma=False,
    )
```

```python
import functools

import jax
import jax.numpy as jnp
from jax import lax
from jax.experimental import pallas as pl
from jax.experimental.pallas import tpu as pltpu
from jax.sharding import PartitionSpec as P

MESH = pl.DeviceIdType.MESH
EPSILON = 1e-06
STAGES = 6
EARLY = 2


def partner(y, step, ny):
    out, bit = 0, 1
    while bit < ny:
        out = out + bit * ((y // bit + step // bit) % 2)
        bit *= 2
    return out


def kernel(n, ny, width, tok_ref, gain_hbm, w_hbm, out_ref, w_s, gat, gain_s, stat, recv, acc, stg,
           cen, coef, gw, fin, tok_sem, gain_sem, w_sem, stat_send, stat_recv, gw_send, gw_recv, gat_send, gat_recv,
           send_sem, recv_sem, met):
    z, y = lax.axis_index("gx"), lax.axis_index("gy")
    tok, depth = tok_ref.shape
    part = tok // n
    stages = stg.shape[0]
    slots = recv.shape[1]
    columns = w_hbm.shape[1]
    tiles = columns // width
    chunks = ny * tiles
    ring = acc.shape[0]
    model = depth * n

    def cols(tile, piece=slice(0, width)):
        if tiles == 1:
            return piece
        return pl.ds(pl.multiple_of(tile * width + piece.start, 128), piece.stop - piece.start)

    def w_copy(tile):
        return pltpu.make_async_copy(w_hbm.at[:, cols(tile)], w_s.at[tile], w_sem.at[tile])

    edges = (0, 384, width) if width > 384 else (0, width)
    pieces = [slice(lo, hi) for lo, hi in zip(edges, edges[1:])]

    def w_piece(i):
        return pltpu.make_async_copy(
            w_hbm.at[:, pieces[i]], w_s.at[0, :, pieces[i]], w_sem.at[tiles if i else 0])

    def rows(plane):
        return pl.ds(pl.multiple_of(plane * part, part), part)

    order = [jnp.where(2 * z < n, n - 1 - i, i) for i in range(n)]

    def tok_copy(i):
        return pltpu.make_async_copy(tok_ref.at[rows(order[i])], gat.at[0, rows(order[i])], tok_sem.at[i])

    for i in range(n):
        tok_copy(i).start()
    gain_copy = pltpu.make_async_copy(gain_hbm, gain_s, gain_sem)
    gain_copy.start()
    w_piece(0).start()

    bits = (ny - 1).bit_length()
    degree = (z > 0).astype(jnp.int32) + (z < n - 1).astype(jnp.int32) + bits

    def greet(sem):
        @pl.when(z > 0)
        def _():
            pl.semaphore_signal(sem, inc=1, device_id=(z - 1, y), device_id_type=MESH)

        @pl.when(z < n - 1)
        def _():
            pl.semaphore_signal(sem, inc=1, device_id=(z + 1, y), device_id_type=MESH)

        for bit in range(bits):
            pl.semaphore_signal(sem, inc=1, device_id=(z, partner(y, 1 << bit, ny)), device_id_type=MESH)

    barrier = pltpu.get_barrier_semaphore()
    greet(barrier)

    def gain_row():
        return gain_s[...].reshape(1, depth)

    def across(ref, send, get, k, slot):
        return pltpu.make_async_remote_copy(
            src_ref=ref.at[slot], dst_ref=ref.at[slot], send_sem=send.at[k], recv_sem=get.at[k],
            device_id=((z + k) % n, y), device_id_type=MESH)

    def gat_copy(k):
        return pltpu.make_async_remote_copy(
            src_ref=gat.at[0], dst_ref=gat.at[k], send_sem=gat_send.at[k], recv_sem=gat_recv.at[k],
            device_id=(z, partner(y, k, ny)), device_id_type=MESH)

    def z_copy(stage, index, slot, chunk, to):
        return pltpu.make_async_remote_copy(
            src_ref=stg.at[stage, index], dst_ref=recv.at[slot, chunk % slots], send_sem=send_sem.at[stage, index],
            recv_sem=recv_sem.at[slot, chunk % slots], device_id=(to, y), device_id_type=MESH)

    last = chunks - 1
    cut = (width - 256) // 128 * 128
    ends = [slice(0, cut), slice(cut, width)] if cut > 0 else [slice(0, width)]

    def end_copy(index, slot, i, to):
        return pltpu.make_async_remote_copy(
            src_ref=stg.at[last % stages, index, :, ends[i]], dst_ref=recv.at[slot, last % slots, :, ends[i]],
            send_sem=send_sem.at[last % stages, index], recv_sem=recv_sem.at[slot, slots if i else last % slots],
            device_id=(to, y), device_id_type=MESH)

    def arrived(slot, chunk):
        pltpu.make_async_remote_copy(
            src_ref=recv.at[slot, chunk % slots], dst_ref=recv.at[slot, chunk % slots], send_sem=send_sem.at[0, 0],
            recv_sem=recv_sem.at[slot, chunk % slots], device_id=((z + 1) % n, y), device_id_type=MESH).wait_recv()

    def landed(slot, chunk):
        return recv[slot, chunk % slots].astype(jnp.float32)

    def forward(chunk, plane, index, out_slot, in_slot, first, to, whole):
        stage = chunk % stages

        @pl.when(chunk >= stages)
        def _():
            z_copy(stage, index, out_slot, chunk, to).wait_send()

        @pl.when(first)
        def _():
            stg[stage, index] = acc[chunk % ring, rows(plane), :]

        @pl.when(jnp.logical_not(first))
        def _():
            arrived(in_slot, chunk)
            stg[stage, index] = (
                acc[chunk % ring, rows(plane), :].astype(jnp.float32) + landed(in_slot, chunk)
            ).astype(jnp.bfloat16)

        if whole:
            z_copy(stage, index, out_slot, chunk, to).start()
        else:
            for i in range(len(ends)):
                end_copy(index, out_slot, i, to).start()

    def right_stage(chunk, j, whole=True):
        forward(chunk, z + 1 + j, j, j, j + 1, z == 0, z + 1, whole)

    def left_stage(chunk, j, whole=True):
        forward(chunk, z - 1 - j, n - 2 - j, n - j, n - 1 - j, z == n - 1, z - 1, whole)

    def open_stage(plane, index, slot, piece, to):
        stg[0, index, :, piece] = acc[0, rows(plane), piece]
        pltpu.make_async_remote_copy(
            src_ref=stg.at[0, index, :, piece], dst_ref=recv.at[slot, 0, :, piece], send_sem=send_sem.at[0, index],
            recv_sem=recv_sem.at[slot, 0], device_id=(to, y), device_id_type=MESH).start()

    gain_copy.wait()
    lane = lax.broadcasted_iota(jnp.int32, (part, 128), 1)
    for i in range(n):
        mine = rows(order[i])
        tok_copy(i).wait()
        if i == 0 and len(pieces) > 1:
            w_piece(1).start()
        values = gat[0, mine, :].astype(jnp.float32)
        total = jnp.sum(values, axis=1, keepdims=True)
        off = values - total / depth
        squares = jnp.sum(off * off, axis=1, keepdims=True)
        coef[mine, :] = jnp.where(lane == 0, total, squares)
        cen[mine, :] = (off * gain_row()).astype(jnp.bfloat16)
        if i == 0:
            w_piece(0).wait()
        acc[0, mine, pieces[0]] = jnp.dot(
            cen[mine, :], w_s[0, :, pieces[0]], preferred_element_type=jnp.float32).astype(jnp.bfloat16)
        if i == 0:
            pl.semaphore_wait(barrier, degree)
            greet(met.at[0])
        if i < n - 1:
            @pl.when(z == 0)
            def _():
                open_stage(n - 1 - i, n - 2 - i, n - 2 - i, pieces[0], 1)

            @pl.when(z == n - 1)
            def _():
                open_stage(i, i, i + 2, pieces[0], n - 2)

    def near(k):
        return jnp.abs((z + k) % n - z) == 1

    stat[z] = coef[...].T[:2]
    for k in range(1, n):
        @pl.when(near(k))
        def _():
            across(stat, stat_send, stat_recv, k, z).start()

    rounds = met.shape[0]
    for r in range(1, rounds):
        pl.semaphore_wait(met.at[r - 1], degree)
        greet(met.at[r])

    if len(pieces) > 1:
        w_piece(1).wait()
    for tile in range(1, tiles):
        w_copy(tile).start()
    for piece in pieces[1:]:
        acc[0, :, piece] = jnp.dot(
            cen[...], w_s[0, :, piece], preferred_element_type=jnp.float32).astype(jnp.bfloat16)

        @pl.when(z == 0)
        def _():
            for j in reversed(range(n - 1)):
                open_stage(1 + j, j, j, piece, 1)

        @pl.when(z == n - 1)
        def _():
            for j in reversed(range(n - 1)):
                open_stage(n - 2 - j, n - 2 - j, n - j, piece, n - 2)

    pl.semaphore_wait(met.at[rounds - 1], degree)
    for k in range(1, n):
        @pl.when(jnp.logical_not(near(k)))
        def _():
            across(stat, stat_send, stat_recv, k, z).start()

    early = min(EARLY, tiles)
    gain = gain_row()
    high = gain.astype(jnp.bfloat16).astype(jnp.float32)
    term = lax.broadcasted_iota(jnp.int32, (16, depth), 0)
    pair = jnp.where(term == 0, high, jnp.where(term == 1, gain - high, 0.0)).astype(jnp.bfloat16)
    for tile in range(early):
        if tile > 0:
            w_copy(tile).wait()
        both = jnp.dot(pair, w_s[tile], preferred_element_type=jnp.float32)
        gw[z, :, tile * width:(tile + 1) * width] = both[0:1] + both[1:2]
    def gw_copy(source, side):
        return pltpu.make_async_remote_copy(
            src_ref=gw.at[source], dst_ref=gw.at[source], send_sem=gw_send.at[side, source],
            recv_sem=gw_recv.at[source], device_id=(z + 1 if side else z - 1, y), device_id_type=MESH)

    def to_right(hop):
        return jnp.logical_and(z >= hop, z < n - 1)

    def to_left(hop):
        return jnp.logical_and(z + hop < n, z > 0)

    def hand_on(hop):
        @pl.when(to_right(hop))
        def _():
            if hop > 0:
                gw_copy(z - hop, 1).wait_recv()
            gw_copy(z - hop, 1).start()

        @pl.when(to_left(hop))
        def _():
            if hop > 0:
                gw_copy(z + hop, 0).wait_recv()
            gw_copy(z + hop, 0).start()

    hand_on(0)

    for tile in range(1, early):
        acc[tile] = jnp.dot(cen[...], w_s[tile], preferred_element_type=jnp.float32).astype(jnp.bfloat16)

        @pl.when(z == 0)
        def _():
            for j in reversed(range(n - 1)):
                right_stage(jnp.int32(tile), j)

        @pl.when(z == n - 1)
        def _():
            for j in reversed(range(n - 1)):
                left_stage(jnp.int32(tile), j)

    for k in range(1, n):
        across(stat, stat_send, stat_recv, k, (z + n - k) % n).wait_recv()
    sums = [stat[k, 0:1, :] for k in range(n)]
    mean = functools.reduce(lambda a, b: a + b, sums) / model
    spread = jnp.zeros_like(mean)
    for k in range(n):
        shift = sums[k] / depth - mean
        spread = spread + stat[k, 1:2, :] + depth * shift * shift
    rstd = lax.rsqrt(spread / model + EPSILON)
    line = lax.broadcasted_iota(jnp.int32, (128, tok), 0)
    table = jnp.where(line == n, rstd, mean)
    for k in range(n):
        table = jnp.where(line == k, (sums[k] / depth - mean) * rstd, table)
    coef[...] = table.T
    gat[0] = (
        (gat[0].astype(jnp.float32) - coef[:, n + 1:n + 2]) * coef[:, n:n + 1] * gain_row()
    ).astype(jnp.bfloat16)
    for k in range(1, ny):
        gat_copy(k).start()

    block = min(part, max(16, 256 // ny))

    def place(chunk, value, piece=slice(0, width)):
        group, tile = chunk // tiles, chunk % tiles
        row = lax.broadcasted_iota(jnp.int32, (block * ny, block), 0)
        col = lax.broadcasted_iota(jnp.int32, (block * ny, block), 1)
        take = (row == col * ny + partner(y, group, ny)).astype(jnp.bfloat16)
        for b in range(part // block):
            moved = jnp.dot(
                take, value[b * block:(b + 1) * block], preferred_element_type=jnp.float32).astype(jnp.bfloat16)
            span = slice(b * block * ny, (b + 1) * block * ny)

            @pl.when(group == 0)
            def _():
                out_ref[span, cols(tile, piece)] = moved

            @pl.when(group > 0)
            def _():
                out_ref[span, cols(tile, piece)] += moved

    def settle(chunk, wait, piece=slice(0, width)):
        mine = acc[chunk % ring, rows(z), piece].astype(jnp.float32)

        def there(slot):
            return recv[slot, chunk % slots, :, piece].astype(jnp.float32)

        @pl.when(z == 0)
        def _():
            wait(n)
            fin[:, piece] = mine + there(n)

        @pl.when(z == n - 1)
        def _():
            wait(0)
            fin[:, piece] = mine + there(0)

        @pl.when(jnp.logical_and(z > 0, z < n - 1))
        def _():
            wait(0)
            wait(n)
            fin[:, piece] = mine + there(0) + there(n)

    @pl.loop(1, chunks + n - 3)
    def _(it):
        @pl.when(jnp.logical_and(it >= early, it < chunks))
        def _():
            tile, group = it % tiles, it // tiles

            @pl.when(group == 0)
            def _():
                w_copy(tile).wait()

            @pl.when(jnp.logical_and(group > 0, tile == 0))
            def _():
                gat_copy(group).wait_recv()

            acc[it % ring] = jnp.dot(gat[group], w_s[tile], preferred_element_type=jnp.float32).astype(jnp.bfloat16)

        for j in reversed(range(n - 1)):
            chunk = it - (n - 2 - j)
            inside = jnp.logical_and(chunk >= 0, chunk < chunks)
            later = jnp.logical_and(chunk >= early, chunk < chunks)

            left = jnp.logical_and(z - 1 - j >= 0, jnp.where(z == n - 1, later, inside))

            @pl.when(jnp.logical_and(left, 2 * z < n))
            def _():
                left_stage(chunk, j)

            @pl.when(jnp.logical_and(z + 1 + j < n, jnp.where(z == 0, later, inside)))
            def _():
                right_stage(chunk, j)

            @pl.when(jnp.logical_and(left, 2 * z >= n))
            def _():
                left_stage(chunk, j)

        own = it - (n - 1)

        @pl.when(own >= 0)
        def _():
            settle(own, lambda slot: arrived(slot, own))

        for tile in range(early):
            @pl.when(own == tile)
            def _():
                if tile == 0:
                    @pl.when(z == 0)
                    def _():
                        for k in range(1, n):
                            gw_copy(k, 1).wait_recv()

                    @pl.when(z == n - 1)
                    def _():
                        for k in range(n - 1):
                            gw_copy(k, 0).wait_recv()

                mine = coef[rows(z), :]
                value = fin[...] * mine[:, n:n + 1]
                for k in range(n):
                    value = value + mine[:, k:k + 1] * gw[k, :, tile * width:(tile + 1) * width]
                fin[...] = value

        @pl.when(own >= 0)
        def _():
            place(own, fin[...].astype(jnp.bfloat16))

        for hop in range(1, n - 1):
            @pl.when(it == hop)
            def _():
                hand_on(hop)

    @pl.when(jnp.logical_and(z > 0, 2 * z < n))
    def _():
        left_stage(last, 0, False)

    @pl.when(z < n - 1)
    def _():
        right_stage(last, 0, False)

    @pl.when(2 * z >= n)
    def _():
        left_stage(last, 0, False)

    settle(last - 1, lambda slot: arrived(slot, last - 1))
    place(last - 1, fin[...].astype(jnp.bfloat16))
    for i, piece in enumerate(ends):
        settle(last, lambda slot: end_copy(0, slot, i, (z + 1) % n).wait_recv(), piece)
        place(last, fin[:, piece].astype(jnp.bfloat16), piece)

    for chunk in range(chunks - stages, chunks):
        for index in range(n - 1):
            z_copy(chunk % stages, index, 0, chunk, (z + 1) % n).wait_send()
    for k in range(1, n):
        across(stat, stat_send, stat_recv, k, z).wait_send()
    for hop in range(n - 1):
        @pl.when(to_right(hop))
        def _():
            gw_copy(z - hop, 1).wait_send()

        @pl.when(to_left(hop))
        def _():
            gw_copy(z + hop, 0).wait_send()

    for k in range(1, ny):
        gat_copy(k).wait_send()


def tile_width(columns, most=7):
    if columns % 128:
        return columns
    lanes = columns // 128
    return 128 * max(k for k in range(1, most + 1) if lanes % k == 0)


def solution(mesh):
    n, ny = mesh.shape["gx"], mesh.shape["gy"]

    def body(tokens, norm_gain, joined_weight):
        tok, depth = tokens.shape
        columns = joined_weight.shape[1]
        part, width = tok // n, tile_width(columns)
        tiles = columns // width
        dma = pltpu.SemaphoreType.DMA
        out = pl.pallas_call(
            functools.partial(kernel, n, ny, width),
            out_shape=pltpu.VMEM((part * ny, columns), jnp.bfloat16),
            in_specs=[pl.BlockSpec(memory_space=pl.ANY)] * 3,
            out_specs=pl.BlockSpec(memory_space=pltpu.VMEM),
            scratch_shapes=[
                pltpu.VMEM((tiles, depth, width), jnp.bfloat16),
                pltpu.VMEM((ny, tok, depth), jnp.bfloat16),
                pltpu.VMEM((depth,), jnp.float32),
                pltpu.VMEM((n + 8, 2, tok), jnp.float32),
                pltpu.VMEM((n + 1, n + 1, part, width), jnp.bfloat16),
                pltpu.VMEM((n, tok, width), jnp.bfloat16),
                pltpu.VMEM((STAGES, n - 1, part, width), jnp.bfloat16),
                pltpu.VMEM((tok, depth), jnp.bfloat16),
                pltpu.VMEM((tok, 128), jnp.float32),
                pltpu.VMEM((n + 8, 1, min(EARLY, tiles) * width), jnp.float32),
                pltpu.VMEM((part, width), jnp.float32),
                dma((n,)), dma, dma((tiles + 1,)), dma((n,)), dma((n,)), dma((2, n)), dma((n,)),
                dma((ny,)), dma((ny,)),
                dma((STAGES, n - 1)), dma((n + 1, n + 2)),
                pltpu.SemaphoreType.REGULAR((max(n - 1, (ny - 1).bit_length()) - 1,)),
            ],
            compiler_params=pltpu.CompilerParams(
                collective_id=0, has_side_effects=True, vmem_limit_bytes=58 * 2 ** 20),
        )(tokens, norm_gain, joined_weight)
        return out.reshape(part, ny, columns)

    return jax.shard_map(
        body,
        mesh=mesh,
        in_specs=(P("gy", "gx"), P("gx"), P("gx", "gy")),
        out_specs=P("gx", None, "gy"),
        check_vma=False,
    )
```
